32 devices in a mesh: dp: 16 (over z, x, core), expert: 2 (over y).
Axes of the slice: x: 2, y: 2, z: 4, core: 2. Of those that a mesh axis runs over, the one named last changes fastest.
Arguments:
- x_rows: bfloat16 [16384, 1024], P(('dp', 'expert')), may hold values from -6 to 6
- dy_rows: bfloat16 [16384, 2048], P(('dp', 'expert')), may hold values from -0.0625 to 0.0625
- seg_blocks: int32 [32, 2], replicated, may hold values from 0 to 2, as said below
Outputs:
- expert_grad: float32 [2, 1024, 2048], P(None, 'dp', 'expert')
The draws below stay inside these ranges and needn't reach their ends.
Inputs may be any that keep to these rules, and one draw needn't show every extreme that they name: `seg_blocks`: on every device the entries sum to at most 4; one expert has exactly 2 blocks on every device.
All inputs are finite; a program needn't handle non-finite values.
Results may differ from the reference program's by a relative error of at most 0.0003.
Values may be sent and summed in bfloat16 or wider, within the bound.
No kernel may reach another device: no remote copies, remote signals or barrier semaphores. Data moves between devices by JAX's collectives and lax.ppermute only.
A program may use at most 128 MiB of HBM per device.

```python
import jax
import jax.numpy as jnp
from jax import lax

H = 1024
F = 2048
BLOCK = 128
CAP = 2
BLOCKS_DEV = 4
EXPERTS = 2
SHARDS = 32
ROWS = 16384


def draw_seg_blocks(key, part):
    hot = jax.random.randint(jax.random.fold_in(key, 7), (), 0, EXPERTS)
    room = min(BLOCKS_DEV, CAP * EXPERTS) - CAP
    experts_row = jnp.arange(EXPERTS, dtype=jnp.int32)

    def single(device):
        sub = jax.random.fold_in(jax.random.fold_in(key, 11), device)
        order = jax.random.permutation(sub, CAP * EXPERTS)
        slot_expert = (order // CAP).astype(jnp.int32)
        others = (slot_expert != hot).astype(jnp.int32)
        rank = jnp.cumsum(others) - 1
        taken = jax.random.randint(jax.random.fold_in(sub, 3), (), room // 2, room + 1)
        chosen = others * (rank < taken).astype(jnp.int32)
        counts = jnp.sum(chosen[:, None] * (slot_expert[:, None] == experts_row[None, :]).astype(jnp.int32), axis=0)
        return (counts + CAP * (experts_row == hot).astype(jnp.int32)).astype(jnp.int32)
    return jax.vmap(single)(jnp.arange(SHARDS, dtype=jnp.int32))


def strengthened(values, own_key, source, target, shards_of, factor):
    owner, partner = [(jnp.arange(values.shape[dim]) // (values.shape[dim] // shards_of)).reshape([-1 if axis == dim else 1 for axis in range(values.ndim)]) for dim in (source, target)]
    chosen = jax.random.permutation(own_key, shards_of)[partner]
    strong = (owner == chosen) | (owner == (partner + shards_of // 2) % shards_of)
    return jnp.where(strong, factor * values, values)


def steps_of(key, extent, shards, least, largest):
    level, own = 1.0, jax.random.fold_in(key, 6)
    for position, blocks in shards:
        draws = jnp.exp(jax.random.uniform(jax.random.fold_in(own, position), (blocks,), jnp.float32, least / len(shards), largest / len(shards)))
        level = level * jnp.repeat(draws, extent[position] // blocks).reshape([-1 if axis == position else 1 for axis in range(len(extent))])
    return level


def scatter_about(own_key, shape, width, limit, cuts=(), kind=jnp.bfloat16):
    values = width * jax.random.normal(own_key, shape, jnp.float32)
    if cuts:
        values = values * steps_of(own_key, shape, cuts, -0.22, 0.18)
    return jnp.clip(values, -limit, limit).astype(kind)


def gaussian_with(own_key, extent, deviation, bound, cuts, heavy, kind=jnp.bfloat16):
    array = deviation * jax.random.normal(own_key, extent, jnp.float32)
    if cuts:
        array = array * steps_of(own_key, extent, cuts, -0.22, 0.18)
    return jnp.clip(strengthened(array, jax.random.fold_in(own_key, 3), *heavy), -bound, bound).astype(kind)


def setup_inputs(seed: int = 0) -> dict:
    keys = jax.random.split(jax.random.key(seed), 4)
    return {
        "x_rows": gaussian_with(keys[0], (ROWS, H), 1.0, 6.0, ((0, 32),), (0, 1, 32, 2.75)),
        "dy_rows": scatter_about(keys[1], (ROWS, F), (SHARDS * CAP * BLOCK) ** -0.5, 0.0625, ((0, 32),)),
        "seg_blocks": draw_seg_blocks(jax.random.fold_in(keys[3], 71), 0),
    }


def pack(xdev, dydev, counts):
    nblk = xdev.shape[0] // BLOCK
    counts = counts.astype(jnp.int32)
    starts = (jnp.cumsum(counts) - counts).astype(jnp.int32)
    slots = jnp.arange(CAP, dtype=jnp.int32)
    live = slots[None, :] < counts[:, None]
    index = jnp.where(live, starts[:, None] + slots[None, :], 0).reshape(-1).astype(jnp.int32)
    keep = live.reshape(-1)[:, None, None]
    xblk = jnp.where(keep, xdev.reshape(nblk, BLOCK, -1)[index], jnp.zeros((), xdev.dtype))
    dyblk = jnp.where(keep, dydev.reshape(nblk, BLOCK, -1)[index], jnp.zeros((), dydev.dtype))
    return xblk, dyblk


def reference(x_rows, dy_rows, seg_blocks):
    xs = x_rows.reshape(SHARDS, -1, H)
    dys = dy_rows.reshape(SHARDS, -1, F)

    def step(total, item):
        xdev, dydev, counts = item
        xblk, dyblk = pack(xdev, dydev, counts)
        xblk = xblk.reshape(EXPERTS, CAP * BLOCK, H).astype(jnp.float32)
        dyblk = dyblk.reshape(EXPERTS, CAP * BLOCK, F).astype(jnp.float32)
        return total + jnp.einsum("erh,erf->ehf", xblk, dyblk), None

    init = jnp.zeros((EXPERTS, H, F), jnp.float32)
    total, _ = lax.scan(step, init, (xs, dys, seg_blocks))
    return total
```

```python
import functools

import jax
import jax.numpy as jnp
from jax import lax
from jax.experimental import pallas as pl
from jax.experimental.pallas import tpu as pltpu
from jax.sharding import PartitionSpec as P

BLOCK = 128
CAP = 2
CHUNKS = 2
LEVELS = 32767.0
TINY = 1e-30


def encode(value):
    top = jnp.maximum(jnp.max(jnp.abs(value), axis=0, keepdims=True), TINY)
    code = jnp.round(value * (LEVELS / top)).astype(jnp.int32).astype(jnp.int16)
    return code, top * (1.0 / LEVELS)


def decode(code, scale):
    return code.astype(jnp.int32).astype(jnp.float32) * scale


def product_kernel(n_src, nz, blk, meta, *refs):
    xs, dys = refs[:n_src], refs[n_src : 2 * n_src]
    code, scale, keep, left = refs[2 * n_src :]
    rows = xs[0].shape[0]
    half = nz * blk

    @pl.when(pl.program_id(0) == 0)
    def _():
        core, x_pos = meta[0], meta[1]
        for s in range(n_src):
            for part in range(2):
                for z in range(nz):
                    x_of = (1 - x_pos) if part == 0 else x_pos
                    col = ((z * 2 + x_of) * 2 + core) * blk
                    tile = pl.multiple_of((col // 128) * 128, 128)
                    sub = (col % 128) // blk
                    for b in range(rows // BLOCK):
                        live = meta[2 + s * (rows // BLOCK) + b]
                        block = xs[s][b * BLOCK : (b + 1) * BLOCK, pl.ds(tile, 128)].T
                        picked = block[:blk]
                        for k in range(1, 128 // blk):
                            picked = jnp.where(sub == k, block[k * blk : (k + 1) * blk], picked)
                        picked = jnp.where(live > 0, picked, jnp.zeros_like(picked))
                        left[
                            part * half + z * blk : part * half + (z + 1) * blk,
                            s * rows + b * BLOCK : s * rows + (b + 1) * BLOCK,
                        ] = picked

    def dot(lo, hi):
        total = None
        for s in range(n_src):
            term = jnp.dot(left[lo:hi, s * rows : (s + 1) * rows], dys[s][...], preferred_element_type=jnp.float32)
            total = term if total is None else total + term
        return total

    sent = dot(0, half)
    for z in range(nz):
        c, s = encode(sent[z * blk : (z + 1) * blk])
        code[z * blk : (z + 1) * blk, :] = c
        scale[z : z + 1, :] = s
    keep[...] = dot(half, 2 * half)


def product(meta, xs, dys, nz, blk, tile=256):
    n_src, (rows, hid), fc = len(xs), xs[0].shape, dys[0].shape[1]
    tile = min(tile, fc)
    half = nz * blk
    return pl.pallas_call(
        functools.partial(product_kernel, n_src, nz, blk),
        grid=(fc // tile,),
        in_specs=[pl.BlockSpec(memory_space=pltpu.SMEM)]
        + [pl.BlockSpec((rows, hid), lambda i: (0, 0))] * n_src
        + [pl.BlockSpec((rows, tile), lambda i: (0, i))] * n_src,
        out_specs=[
            pl.BlockSpec((half, tile), lambda i: (0, i)),
            pl.BlockSpec((nz, tile), lambda i: (0, i)),
            pl.BlockSpec((half, tile), lambda i: (0, i)),
        ],
        out_shape=[
            jax.ShapeDtypeStruct((half, fc), jnp.int16),
            jax.ShapeDtypeStruct((nz, fc), jnp.float32),
            jax.ShapeDtypeStruct((half, fc), jnp.float32),
        ],
        scratch_shapes=[pltpu.VMEM((2 * half, n_src * rows), jnp.bfloat16)],
        cost_estimate=pl.CostEstimate(
            flops=4 * half * fc * n_src * rows, bytes_accessed=n_src * rows * (hid + fc) * 2, transcendentals=0
        ),
        name="product",
    )(meta, *xs, *dys)


def middle_kernel(nz, blk, meta, code, scale, keep, *outs):
    z_pos = meta[0]
    own = outs[-1]
    for j in range(nz):
        z = lax.rem(z_pos + j, nz)
        at = pl.ds(pl.multiple_of(z * blk, blk), blk)
        value = keep[at, :] + decode(code[at, :], scale[pl.ds(z, 1), :])
        if j == 0:
            own[...] = value
        else:
            c, s = encode(value)
            outs[2 * (j - 1)][...] = c
            outs[2 * (j - 1) + 1][...] = s


def middle(meta, code, scale, keep, nz, blk, tile=512):
    fc = code.shape[1]
    tile = min(tile, fc)
    shapes, specs = [], []
    for _ in range(nz - 1):
        shapes += [jax.ShapeDtypeStruct((blk, fc), jnp.int16), jax.ShapeDtypeStruct((1, fc), jnp.float32)]
        specs += [pl.BlockSpec((blk, tile), lambda i: (0, i)), pl.BlockSpec((1, tile), lambda i: (0, i))]
    shapes.append(jax.ShapeDtypeStruct((blk, fc), jnp.float32))
    specs.append(pl.BlockSpec((blk, tile), lambda i: (0, i)))
    return pl.pallas_call(
        functools.partial(middle_kernel, nz, blk),
        grid=(fc // tile,),
        in_specs=[
            pl.BlockSpec(memory_space=pltpu.SMEM),
            pl.BlockSpec((nz * blk, tile), lambda i: (0, i)),
            pl.BlockSpec((nz, tile), lambda i: (0, i)),
            pl.BlockSpec((nz * blk, tile), lambda i: (0, i)),
        ],
        out_specs=specs,
        out_shape=shapes,
        cost_estimate=pl.CostEstimate(flops=nz * blk * fc * 8, bytes_accessed=nz * blk * fc * 8, transcendentals=0),
        name="middle",
    )(meta, code, scale, keep)


def total_kernel(nz, own, *refs):
    value = own[...]
    for j in range(nz - 1):
        value = value + decode(refs[2 * j][...], refs[2 * j + 1][...])
    refs[-1][...] = value


def place_kernel(nz, meta, own, *refs):
    value = own[...]
    for j in range(nz - 1):
        value = value + decode(refs[2 * j][...], refs[2 * j + 1][...])
    other, out = refs[-2], refs[-1]
    me = meta[0]
    out[me] = value
    out[1 - me] = other[...]


def total(own, coded, nz):
    return pl.pallas_call(
        functools.partial(total_kernel, nz),
        out_shape=jax.ShapeDtypeStruct(own.shape, jnp.float32),
        cost_estimate=pl.CostEstimate(flops=own.size * 8, bytes_accessed=own.size * 8, transcendentals=0),
        name="total",
    )(own, *coded)


def place(meta, own, coded, other, nz):
    vmem = pl.BlockSpec(memory_space=pltpu.VMEM)
    return pl.pallas_call(
        functools.partial(place_kernel, nz),
        in_specs=[pl.BlockSpec(memory_space=pltpu.SMEM)] + [vmem] * (2 + len(coded)),
        out_specs=vmem,
        out_shape=jax.ShapeDtypeStruct((2, *own.shape), jnp.float32),
        cost_estimate=pl.CostEstimate(flops=own.size * 8, bytes_accessed=own.size * 8, transcendentals=0),
        name="place",
    )(meta, own, *coded, other)


def shards(x_rows, dy_rows, seg_blocks):
    rows, hid = x_rows.shape
    ffn = dy_rows.shape[1]
    n_exp = lax.axis_size("expert")
    n_dp = lax.axis_size("dp")
    nblk = rows // BLOCK
    cap = min(CAP, nblk)
    blk = hid // n_dp
    nz = n_dp // 4
    piece = ffn // n_exp
    per_chunk = n_exp // CHUNKS
    e = lax.axis_index("expert")
    d = lax.axis_index("dp")
    core, x_pos, z_pos = d % 2, (d // 2) % 2, d // 4

    def first_of(starts):
        return jnp.minimum(starts, nblk - cap)

    counts_all = seg_blocks
    starts_all = jnp.cumsum(counts_all, axis=1) - counts_all

    def live_of(dp_pos, e_pos):
        row = dp_pos * n_exp + e_pos
        start, count = starts_all[row, e], counts_all[row, e]
        block = first_of(start) + jnp.arange(cap, dtype=jnp.int32)
        return ((block >= start) & (block < start + count)).astype(jnp.int32)

    def segment(expert):
        start = first_of(starts_all[d * n_exp + e, expert]) * BLOCK
        xs = lax.dynamic_slice(x_rows, (start, 0), (cap * BLOCK, hid))
        dys = []
        for chunk in range(CHUNKS):
            pieces = []
            for p in range(per_chunk):
                column = ((expert + 1 + chunk * per_chunk + p) % n_exp) * piece
                pieces.append(lax.dynamic_slice(dy_rows, (start, column), (cap * BLOCK, piece)))
            dys.append(pieces[0] if per_chunk == 1 else jnp.concatenate(pieces, axis=1))
        return xs, dys

    swap = [(i, i ^ 1) for i in range(n_dp)]
    xs, dys, live = [], [[] for _ in range(CHUNKS)], []
    for j in range(n_exp):
        sx, sdy = segment((e + j) % n_exp)
        if j:
            ring = [(i, (i + j) % n_exp) for i in range(n_exp)]
            sx = lax.ppermute(sx, "expert", ring)
            sdy = [lax.ppermute(a, "expert", ring) for a in sdy]
        origin = (e - j) % n_exp
        xs += [sx, lax.ppermute(sx, "dp", swap)]
        for chunk in range(CHUNKS):
            dys[chunk] += [sdy[chunk], lax.ppermute(sdy[chunk], "dp", swap)]
        live += [live_of(d, origin), live_of(d ^ 1, origin)]
    meta = jnp.concatenate([jnp.stack([core, x_pos]).astype(jnp.int32), *live])

    over_x = [(i, i ^ 2) for i in range(n_dp)]
    z_meta = z_pos.astype(jnp.int32).reshape(1)
    e_meta = e.astype(jnp.int32).reshape(1)
    got = []
    for chunk in range(CHUNKS):
        code, scale, keep = product(meta, xs, dys[chunk], nz, blk)
        code, scale = lax.ppermute(code, "dp", over_x), lax.ppermute(scale, "dp", over_x)
        *coded, own = middle(z_meta, code, scale, keep, nz, blk)
        for j in range(1, nz):
            ring = [(i, (i + 4 * j) % n_dp) for i in range(n_dp)]
            for k in (2 * j - 2, 2 * j - 1):
                coded[k] = lax.ppermute(coded[k], "dp", ring)
        if n_exp == 2 and chunk == CHUNKS - 1:
            return place(e_meta, own, coded, got[0], nz)
        summed = total(own, coded, nz)
        for p in range(per_chunk):
            shift = 1 + chunk * per_chunk + p
            ring = [(i, (i + shift) % n_exp) for i in range(n_exp)]
            part = summed[:, p * piece : (p + 1) * piece]
            got.append(lax.ppermute(part, "expert", ring) if shift < n_exp else part)
    order = (e - 1 - jnp.arange(n_exp)) % n_exp
    return jnp.stack(got)[order]


def solution(mesh):
    in_specs = (P(("dp", "expert"), None), P(("dp", "expert"), None), P())
    out_specs = P(None, "dp", "expert")
    return jax.shard_map(shards, mesh=mesh, in_specs=in_specs, out_specs=out_specs, check_vma=False)
```

```python
import functools

import jax
import jax.numpy as jnp
from jax import lax
from jax.experimental import pallas as pl
from jax.experimental.pallas import tpu as pltpu
from jax.sharding import PartitionSpec as P

BLOCK = 128
CAP = 2
CHUNKS = 2
LEVELS = 32767.0
TINY = 1e-30
STEPS = 128.0
TILE_ROWS = 16


def exponent_of(value):
    top = jnp.maximum(jnp.max(jnp.abs(value), axis=0, keepdims=True), TINY)
    return jnp.ceil(jnp.log2(top) * STEPS) + 1.0


def bound_of(exponent):
    return jnp.exp2(exponent * (1.0 / STEPS))


def coded(value, exponent):
    return jnp.round(value * (LEVELS / bound_of(exponent))).astype(jnp.int32).astype(jnp.int16)


def decoded(code, exponent):
    scale = bound_of(exponent.astype(jnp.int32).astype(jnp.float32)) * (1.0 / LEVELS)
    return code.astype(jnp.int32).astype(jnp.float32) * scale


def exponent_rows(exponents):
    shape = (TILE_ROWS, exponents[0].shape[1])
    row = lax.broadcasted_iota(jnp.int32, shape, 0)
    rows = jnp.zeros(shape, jnp.int32)
    for k, exponent in enumerate(exponents):
        rows = jnp.where(row == k, exponent.astype(jnp.int32), rows)
    return rows.astype(jnp.int16)


def exponent_at(tile, k):
    return tile.astype(jnp.int32)[k : k + 1]


def first_and_count(seg, row, expert, nblk, cap):
    start = jnp.int32(0)
    for other in range(seg.shape[1]):
        start = start + jnp.where(other < expert, seg[row, other], 0)
    return start, jnp.minimum(start, nblk - cap), seg[row, expert]


def pack_kernel(n_exp, cap, seg, x, dy, own, *sends):
    rows, hid = x.shape
    ffn = dy.shape[1]
    piece = ffn // n_exp
    per_chunk = n_exp // CHUNKS
    fc = ffn // CHUNKS
    e = lax.axis_index("expert")
    me = lax.axis_index("dp") * n_exp + e
    for j in range(n_exp):
        expert = lax.rem(e + j, n_exp)
        _, first, _ = first_and_count(seg, me, expert, rows // BLOCK, cap)
        at = pl.ds(pl.multiple_of(first * BLOCK, BLOCK), cap * BLOCK)
        head = own if j == 0 else sends[2 * j - 2]
        head[:, :hid] = x[at, :]
        for chunk in range(CHUNKS):
            for p in range(per_chunk):
                which = lax.rem(expert + 1 + chunk * per_chunk + p, n_exp)
                block = dy[at, pl.ds(pl.multiple_of(which * piece, 128), piece)]
                if j == 0 or chunk == 0:
                    to = hid + chunk * fc + p * piece
                    head[:, to : to + piece] = block
                else:
                    sends[2 * j - 1][:, p * piece : (p + 1) * piece] = block


def pack(seg, x, dy, n_exp, cap):
    hid, fc = x.shape[1], dy.shape[1] // CHUNKS
    rows = cap * BLOCK
    vmem = pl.BlockSpec(memory_space=pltpu.VMEM)
    shapes = [jax.ShapeDtypeStruct((rows, hid + 2 * fc), x.dtype)]
    for _ in range(n_exp - 1):
        shapes += [jax.ShapeDtypeStruct((rows, hid + fc), x.dtype), jax.ShapeDtypeStruct((rows, fc), x.dtype)]
    return pl.pallas_call(
        functools.partial(pack_kernel, n_exp, cap),
        in_specs=[pl.BlockSpec(memory_space=pltpu.SMEM), vmem, vmem],
        out_specs=[vmem] * len(shapes),
        out_shape=shapes,
        name="pack",
    )(seg, x, dy)


def left_of(n_exp, nblk, nz, blk, seg, xs, left):
    rows = xs[0].shape[0]
    cap = rows // BLOCK
    half = nz * blk
    e, d = lax.axis_index("expert"), lax.axis_index("dp")
    core, x_pos = lax.rem(d, 2), lax.rem(d // 2, 2)
    for s in range(len(xs)):
        origin = lax.rem(e - s // 2 + n_exp, n_exp)
        dp_pos = d if s % 2 == 0 else d + 1 - 2 * core
        start, first, count = first_and_count(seg, dp_pos * n_exp + origin, e, nblk, cap)
        for part in range(2):
            for z in range(nz):
                x_of = (1 - x_pos) if part == 0 else x_pos
                col = ((z * 2 + x_of) * 2 + core) * blk
                tile = pl.multiple_of((col // 128) * 128, 128)
                sub = lax.rem(col, 128) // blk
                for b in range(cap):
                    live = jnp.logical_and(first + b >= start, first + b < start + count)
                    block = xs[s][b * BLOCK : (b + 1) * BLOCK, pl.ds(tile, 128)].T
                    picked = block[:blk]
                    for k in range(1, 128 // blk):
                        picked = jnp.where(sub == k, block[k * blk : (k + 1) * blk], picked)
                    picked = jnp.where(live, picked, jnp.zeros_like(picked))
                    left[
                        part * half + z * blk : part * half + (z + 1) * blk,
                        s * rows + b * BLOCK : s * rows + (b + 1) * BLOCK,
                    ] = picked


def product_body(nz, blk, left, dys, code, keep):
    rows = dys[0].shape[0]
    half = nz * blk

    def dot(lo, hi):
        total = None
        for s, dy in enumerate(dys):
            term = jnp.dot(left[lo:hi, s * rows : (s + 1) * rows], dy[...], preferred_element_type=jnp.float32)
            total = term if total is None else total + term
        return total

    sent = dot(0, half)
    exponents = []
    for z in range(nz):
        block = sent[z * blk : (z + 1) * blk]
        exponents.append(exponent_of(block))
        code[z * blk : (z + 1) * blk, :] = coded(block, exponents[z])
    code[half : half + TILE_ROWS, :] = exponent_rows(exponents)
    keep[...] = dot(half, 2 * half)


def first_kernel(n_exp, nblk, nz, blk, seg, *refs):
    n_src = 2 * n_exp
    xs, dys = refs[:n_src], refs[n_src : 2 * n_src]
    code, keep, left = refs[2 * n_src :]

    @pl.when(pl.program_id(0) == 0)
    def _():
        left_of(n_exp, nblk, nz, blk, seg, xs, left)

    product_body(nz, blk, left, dys, code, keep)


def later_kernel(nz, blk, left, *refs):
    *dys, code, keep = refs
    product_body(nz, blk, left, dys, code, keep)


def product(seg, left, heads, dys, n_exp, nblk, nz, blk, hid, fc, tile=256):
    n_src, rows = len(dys), dys[0][0].shape[0]
    tile = min(tile, fc)
    half = nz * blk
    whole_left = pl.BlockSpec((2 * half, n_src * rows), lambda i: (0, 0))
    dy_specs = [pl.BlockSpec((rows, tile), functools.partial(lambda at, i: (0, at + i), at // tile)) for _, at in dys]
    out_specs = [
        pl.BlockSpec((half + TILE_ROWS, tile), lambda i: (0, i)),
        pl.BlockSpec((half, tile), lambda i: (0, i)),
    ]
    out_shape = [
        jax.ShapeDtypeStruct((half + TILE_ROWS, fc), jnp.int16),
        jax.ShapeDtypeStruct((half, fc), jnp.float32),
    ]
    if left is None:
        kernel = functools.partial(first_kernel, n_exp, nblk, nz, blk)
        in_specs = [pl.BlockSpec(memory_space=pltpu.SMEM)]
        in_specs += [pl.BlockSpec((rows, hid), lambda i: (0, 0))] * n_src
        args = [seg, *heads]
        out_specs.append(whole_left)
        out_shape.append(jax.ShapeDtypeStruct((2 * half, n_src * rows), jnp.bfloat16))
    else:
        kernel, in_specs, args = functools.partial(later_kernel, nz, blk), [whole_left], [left]
    return pl.pallas_call(
        kernel,
        grid=(fc // tile,),
        in_specs=in_specs + dy_specs,
        out_specs=out_specs,
        out_shape=out_shape,
        cost_estimate=pl.CostEstimate(
            flops=4 * half * fc * n_src * rows, bytes_accessed=n_src * rows * (hid + fc) * 2, transcendentals=0
        ),
        name="product",
    )(*args, *[a for a, _ in dys])


def groups_of(fc):
    return max(g for g in (1, 2, 4) if fc % (g * 128) == 0)


def middle_kernel(nz, blk, code, keep, *outs):
    z_pos = lax.axis_index("dp") // 4
    fc = keep.shape[1]
    groups = groups_of(fc)
    wide = fc // groups
    exponent_tile = code[nz * blk : nz * blk + TILE_ROWS, :].astype(jnp.int32)
    row = lax.broadcasted_iota(jnp.int32, exponent_tile.shape, 0)
    for j in range(nz):
        z = lax.rem(z_pos + j, nz)
        at = pl.ds(pl.multiple_of(z * blk, blk), blk)
        exponent = jnp.sum(jnp.where(row == z, exponent_tile, 0), axis=0, keepdims=True)
        value = keep[at, :] + decoded(code[at, :], exponent)
        if j == 0:
            outs[-1][...] = value
            continue
        exponents = []
        for g in range(groups):
            block = value[:, g * wide : (g + 1) * wide]
            exponents.append(exponent_of(block))
            outs[j - 1][g * blk : (g + 1) * blk, :] = coded(block, exponents[g])
        outs[j - 1][groups * blk : groups * blk + TILE_ROWS, :] = exponent_rows(exponents)


def middle(code, keep, nz, blk):
    fc = code.shape[1]
    groups = groups_of(fc)
    vmem = pl.BlockSpec(memory_space=pltpu.VMEM)
    shapes = [jax.ShapeDtypeStruct((groups * blk + TILE_ROWS, fc // groups), jnp.int16)] * (nz - 1)
    shapes.append(jax.ShapeDtypeStruct((blk, fc), jnp.float32))
    return pl.pallas_call(
        functools.partial(middle_kernel, nz, blk),
        in_specs=[vmem, vmem],
        out_specs=[vmem] * nz,
        out_shape=shapes,
        cost_estimate=pl.CostEstimate(flops=nz * blk * fc * 8, bytes_accessed=nz * blk * fc * 8, transcendentals=0),
        name="middle",
    )(code, keep)


def summed_over_z(own, codes):
    blk, fc = own.shape
    groups = groups_of(fc)
    wide = fc // groups
    parts = []
    for g in range(groups):
        value = own[:, g * wide : (g + 1) * wide]
        for ref in codes:
            exponent = exponent_at(ref[groups * blk : groups * blk + TILE_ROWS, :], g)
            value = value + decoded(ref[g * blk : (g + 1) * blk, :], exponent)
        parts.append(value)
    return parts


def total_kernel(own, *refs):
    wide = own.shape[1] // groups_of(own.shape[1])
    for g, value in enumerate(summed_over_z(own, refs[:-1])):
        refs[-1][:, g * wide : (g + 1) * wide] = value


def place_kernel(own, *refs):
    *codes, other, out = refs
    wide = own.shape[1] // groups_of(own.shape[1])
    e = lax.axis_index("expert")
    for g, value in enumerate(summed_over_z(own, codes)):
        out[e, :, g * wide : (g + 1) * wide] = value
    out[1 - e] = other[...]


def total(own, codes):
    vmem = pl.BlockSpec(memory_space=pltpu.VMEM)
    return pl.pallas_call(
        total_kernel,
        in_specs=[vmem] * (1 + len(codes)),
        out_specs=vmem,
        out_shape=jax.ShapeDtypeStruct(own.shape, jnp.float32),
        cost_estimate=pl.CostEstimate(flops=own.size * 8, bytes_accessed=own.size * 8, transcendentals=0),
        name="total",
    )(own, *codes)


def place(own, codes, other):
    vmem = pl.BlockSpec(memory_space=pltpu.VMEM)
    return pl.pallas_call(
        place_kernel,
        in_specs=[vmem] * (2 + len(codes)),
        out_specs=vmem,
        out_shape=jax.ShapeDtypeStruct((2, *own.shape), jnp.float32),
        cost_estimate=pl.CostEstimate(flops=own.size * 8, bytes_accessed=own.size * 8, transcendentals=0),
        name="place",
    )(own, *codes, other)


def shards(x_rows, dy_rows, seg_blocks):
    rows, hid = x_rows.shape
    ffn = dy_rows.shape[1]
    n_exp = lax.axis_size("expert")
    n_dp = lax.axis_size("dp")
    nblk = rows // BLOCK
    cap = min(CAP, nblk)
    blk = hid // n_dp
    nz = n_dp // 4
    piece = ffn // n_exp
    per_chunk = n_exp // CHUNKS
    fc = ffn // CHUNKS

    swap = [(i, i ^ 1) for i in range(n_dp)]
    over_x = [(i, i ^ 2) for i in range(n_dp)]

    def ring(n, j):
        return [(i, (i + j) % n) for i in range(n)]

    own, *sends = pack(seg_blocks, x_rows, dy_rows, n_exp, cap)
    heads = [lax.ppermute(sends[2 * j - 2], "expert", ring(n_exp, j)) for j in range(1, n_exp)]
    tails = [lax.ppermute(sends[2 * j - 1], "expert", ring(n_exp, j)) for j in range(1, n_exp)]
    own_pair = [own, lax.ppermute(own, "dp", swap)]
    head_pairs = []
    for head in heads:
        head_pairs += [head, lax.ppermute(head, "dp", swap)]

    got, left, codes = [], None, []
    for chunk in range(CHUNKS):
        dys = [(a, hid + chunk * fc) for a in own_pair]
        if chunk == 0:
            dys += [(a, hid) for a in head_pairs]
            code, keep, left = product(
                seg_blocks, None, own_pair + head_pairs, dys, n_exp, nblk, nz, blk, hid, fc
            )
        else:
            code0, *tails = lax.optimization_barrier((codes[0][0], *tails))
            codes[0] = (code0, codes[0][1])
            for tail in tails:
                dys += [(tail, 0), (lax.ppermute(tail, "dp", swap), 0)]
            code, keep = product(seg_blocks, left, None, dys, n_exp, nblk, nz, blk, hid, fc)
        codes.append((code, keep))
    for chunk in range(CHUNKS):
        code, keep = codes[chunk]
        *parts, own = middle(lax.ppermute(code, "dp", over_x), keep, nz, blk)
        parts = [lax.ppermute(part, "dp", ring(n_dp, 4 * (j + 1))) for j, part in enumerate(parts)]
        if n_exp == 2 and chunk == CHUNKS - 1:
            return place(own, parts, got[0])
        result = total(own, parts)
        for p in range(per_chunk):
            shift = 1 + chunk * per_chunk + p
            part = result[:, p * piece : (p + 1) * piece]
            got.append(lax.ppermute(part, "expert", ring(n_exp, shift)) if shift < n_exp else part)
    order = (lax.axis_index("expert") - 1 - jnp.arange(n_exp)) % n_exp
    return jnp.stack(got)[order]


def solution(mesh):
    in_specs = (P(("dp", "expert"), None), P(("dp", "expert"), None), P())
    out_specs = P(None, "dp", "expert")
    return jax.shard_map(shards, mesh=mesh, in_specs=in_specs, out_specs=out_specs, check_vma=False)
```

```python
import functools

import jax
import jax.numpy as jnp
from jax import lax
from jax.experimental import pallas as pl
from jax.experimental.pallas import tpu as pltpu
from jax.sharding import PartitionSpec as P


BLOCK = 128
CAP = 2
CHUNKS = 2
LEVELS = 32767.0
TINY = 1e-30
STEPS = 128.0
TILE_ROWS = 16


def exponent_of(value):
    top = jnp.maximum(jnp.max(jnp.abs(value), axis=0, keepdims=True), TINY)
    return jnp.ceil(jnp.log2(top) * STEPS) + 1.0


def bound_of(exponent):
    return jnp.exp2(exponent * (1.0 / STEPS))


def coded(value, exponent):
    return jnp.round(value * (LEVELS / bound_of(exponent))).astype(jnp.int32).astype(jnp.int16)


def decoded(code, exponent):
    scale = bound_of(exponent.astype(jnp.int32).astype(jnp.float32)) * (1.0 / LEVELS)
    return code.astype(jnp.int32).astype(jnp.float32) * scale


def exponent_rows(exponents):
    shape = (TILE_ROWS, exponents[0].shape[1])
    row = lax.broadcasted_iota(jnp.int32, shape, 0)
    rows = jnp.zeros(shape, jnp.int32)
    for k, exponent in enumerate(exponents):
        rows = jnp.where(row == k, exponent.astype(jnp.int32), rows)
    return rows.astype(jnp.int16)


def exponent_at(tile, k):
    return tile.astype(jnp.int32)[k : k + 1]


def first_and_count(seg, row, expert, nblk, cap):
    start = jnp.int32(0)
    for other in range(seg.shape[1]):
        start = start + jnp.where(other < expert, seg[row, other], 0)
    return start, jnp.minimum(start, nblk - cap), seg[row, expert]


def pack_kernel(n_exp, cap, seg, x, dy, own, *sends):
    rows, hid = x.shape
    ffn = dy.shape[1]
    piece = ffn // n_exp
    per_chunk = n_exp // CHUNKS
    fc = ffn // CHUNKS
    e = lax.axis_index("expert")
    me = lax.axis_index("dp") * n_exp + e
    for j in range(n_exp):
        expert = lax.rem(e + j, n_exp)
        _, first, _ = first_and_count(seg, me, expert, rows // BLOCK, cap)
        at = pl.ds(pl.multiple_of(first * BLOCK, BLOCK), cap * BLOCK)
        head = own if j == 0 else sends[2 * j - 2]
        head[:, :hid] = x[at, :]
        for chunk in range(CHUNKS):
            for p in range(per_chunk):
                which = lax.rem(expert + 1 + chunk * per_chunk + p, n_exp)
                block = dy[at, pl.ds(pl.multiple_of(which * piece, 128), piece)]
                if j == 0 or chunk == 0:
                    to = hid + chunk * fc + p * piece
                    head[:, to : to + piece] = block
                else:
                    sends[2 * j - 1][:, p * piece : (p + 1) * piece] = block


def pack(seg, x, dy, n_exp, cap):
    hid, fc = x.shape[1], dy.shape[1] // CHUNKS
    rows = cap * BLOCK
    vmem = pl.BlockSpec(memory_space=pltpu.VMEM)
    shapes = [jax.ShapeDtypeStruct((rows, hid + 2 * fc), x.dtype)]
    for _ in range(n_exp - 1):
        shapes += [jax.ShapeDtypeStruct((rows, hid + fc), x.dtype), jax.ShapeDtypeStruct((rows, fc), x.dtype)]
    return pl.pallas_call(
        functools.partial(pack_kernel, n_exp, cap),
        in_specs=[pl.BlockSpec(memory_space=pltpu.SMEM), vmem, vmem],
        out_specs=[vmem] * len(shapes),
        out_shape=shapes,
        name="pack",
    )(seg, x, dy)


def left_of(n_exp, nblk, nz, blk, seg, xs, left):
    rows = xs[0].shape[0]
    cap = rows // BLOCK
    half = nz * blk
    e, d = lax.axis_index("expert"), lax.axis_index("dp")
    core, x_pos = lax.rem(d, 2), lax.rem(d // 2, 2)
    for s in range(len(xs)):
        origin = lax.rem(e - s // 2 + n_exp, n_exp)
        dp_pos = d if s % 2 == 0 else d + 1 - 2 * core
        start, first, count = first_and_count(seg, dp_pos * n_exp + origin, e, nblk, cap)
        for part in range(2):
            for z in range(nz):
                x_of = (1 - x_pos) if part == 0 else x_pos
                col = ((z * 2 + x_of) * 2 + core) * blk
                tile = pl.multiple_of((col // 128) * 128, 128)
                sub = lax.rem(col, 128) // blk
                for b in range(cap):
                    live = jnp.logical_and(first + b >= start, first + b < start + count)
                    block = xs[s][b * BLOCK : (b + 1) * BLOCK, pl.ds(tile, 128)].T
                    picked = block[:blk]
                    for k in range(1, 128 // blk):
                        picked = jnp.where(sub == k, block[k * blk : (k + 1) * blk], picked)
                    picked = jnp.where(live, picked, jnp.zeros_like(picked))
                    left[
                        part * half + z * blk : part * half + (z + 1) * blk,
                        s * rows + b * BLOCK : s * rows + (b + 1) * BLOCK,
                    ] = picked


def product_body(nz, blk, left, dys, code, keep):
    half = nz * blk
    tokens = jnp.concatenate([dy[...] for dy in dys], axis=0)
    both = jnp.dot(left[...], tokens, preferred_element_type=jnp.float32)
    sent = both[:half]
    exponents = []
    for z in range(nz):
        block = sent[z * blk : (z + 1) * blk]
        exponents.append(exponent_of(block))
        code[z * blk : (z + 1) * blk, :] = coded(block, exponents[z])
    code[half : half + TILE_ROWS, :] = exponent_rows(exponents)
    keep[...] = both[half:]


def first_kernel(n_exp, nblk, nz, blk, seg, *refs):
    n_src = 2 * n_exp
    xs, dys = refs[:n_src], refs[n_src : 2 * n_src]
    code, keep, left = refs[2 * n_src :]

    @pl.when(pl.program_id(0) == 0)
    def _():
        left_of(n_exp, nblk, nz, blk, seg, xs, left)

    product_body(nz, blk, left, dys, code, keep)


def later_kernel(nz, blk, left, *refs):
    *dys, code, keep = refs
    product_body(nz, blk, left, dys, code, keep)


def product(seg, left, heads, dys, n_exp, nblk, nz, blk, hid, fc, tile=256):
    n_src, rows = len(dys), dys[0][0].shape[0]
    tile = min(tile, fc)
    half = nz * blk
    whole_left = pl.BlockSpec((2 * half, n_src * rows), lambda i: (0, 0))
    dy_specs = [pl.BlockSpec((rows, tile), functools.partial(lambda at, i: (0, at + i), at // tile)) for _, at in dys]
    out_specs = [
        pl.BlockSpec((half + TILE_ROWS, tile), lambda i: (0, i)),
        pl.BlockSpec((half, tile), lambda i: (0, i)),
    ]
    out_shape = [
        jax.ShapeDtypeStruct((half + TILE_ROWS, fc), jnp.int16),
        jax.ShapeDtypeStruct((half, fc), jnp.float32),
    ]
    if left is None:
        kernel = functools.partial(first_kernel, n_exp, nblk, nz, blk)
        in_specs = [pl.BlockSpec(memory_space=pltpu.SMEM)]
        in_specs += [pl.BlockSpec((rows, hid), lambda i: (0, 0))] * n_src
        args = [seg, *heads]
        out_specs.append(whole_left)
        out_shape.append(jax.ShapeDtypeStruct((2 * half, n_src * rows), jnp.bfloat16))
    else:
        kernel, in_specs, args = functools.partial(later_kernel, nz, blk), [whole_left], [left]
    return pl.pallas_call(
        kernel,
        grid=(fc // tile,),
        in_specs=in_specs + dy_specs,
        out_specs=out_specs,
        out_shape=out_shape,
        cost_estimate=pl.CostEstimate(
            flops=4 * half * fc * n_src * rows, bytes_accessed=n_src * rows * (hid + fc) * 2, transcendentals=0
        ),
        name="product",
    )(*args, *[a for a, _ in dys])


def groups_of(fc):
    return max(g for g in (1, 2, 4) if fc % (g * 128) == 0)


def middle_kernel(nz, blk, code, keep, *outs):
    z_pos = lax.axis_index("dp") // 4
    fc = keep.shape[1]
    groups = groups_of(fc)
    wide = fc // groups
    exponent_tile = code[nz * blk : nz * blk + TILE_ROWS, :].astype(jnp.int32)
    row = lax.broadcasted_iota(jnp.int32, exponent_tile.shape, 0)
    for j in range(nz):
        z = lax.rem(z_pos + j, nz)
        at = pl.ds(pl.multiple_of(z * blk, blk), blk)
        exponent = jnp.sum(jnp.where(row == z, exponent_tile, 0), axis=0, keepdims=True)
        value = keep[at, :] + decoded(code[at, :], exponent)
        if j == 0:
            outs[-1][...] = value
            continue
        exponents = []
        for g in range(groups):
            block = value[:, g * wide : (g + 1) * wide]
            exponents.append(exponent_of(block))
            outs[j - 1][g * blk : (g + 1) * blk, :] = coded(block, exponents[g])
        outs[j - 1][groups * blk : groups * blk + TILE_ROWS, :] = exponent_rows(exponents)


def middle(code, keep, nz, blk):
    fc = code.shape[1]
    groups = groups_of(fc)
    vmem = pl.BlockSpec(memory_space=pltpu.VMEM)
    shapes = [jax.ShapeDtypeStruct((groups * blk + TILE_ROWS, fc // groups), jnp.int16)] * (nz - 1)
    shapes.append(jax.ShapeDtypeStruct((blk, fc), jnp.float32))
    return pl.pallas_call(
        functools.partial(middle_kernel, nz, blk),
        in_specs=[vmem, vmem],
        out_specs=[vmem] * nz,
        out_shape=shapes,
        cost_estimate=pl.CostEstimate(flops=nz * blk * fc * 8, bytes_accessed=nz * blk * fc * 8, transcendentals=0),
        name="middle",
    )(code, keep)


def summed_over_z(own, codes):
    blk, fc = own.shape
    groups = groups_of(fc)
    wide = fc // groups
    parts = []
    for g in range(groups):
        value = own[:, g * wide : (g + 1) * wide]
        for ref in codes:
            exponent = exponent_at(ref[groups * blk : groups * blk + TILE_ROWS, :], g)
            value = value + decoded(ref[g * blk : (g + 1) * blk, :], exponent)
        parts.append(value)
    return parts


def total_kernel(own, *refs):
    wide = own.shape[1] // groups_of(own.shape[1])
    for g, value in enumerate(summed_over_z(own, refs[:-1])):
        refs[-1][:, g * wide : (g + 1) * wide] = value


def place_kernel(own, *refs):
    *codes, other, out = refs
    wide = own.shape[1] // groups_of(own.shape[1])
    e = lax.axis_index("expert")
    for g, value in enumerate(summed_over_z(own, codes)):
        out[e, :, g * wide : (g + 1) * wide] = value
    out[1 - e] = other[...]


def total(own, codes):
    vmem = pl.BlockSpec(memory_space=pltpu.VMEM)
    return pl.pallas_call(
        total_kernel,
        in_specs=[vmem] * (1 + len(codes)),
        out_specs=vmem,
        out_shape=jax.ShapeDtypeStruct(own.shape, jnp.float32),
        cost_estimate=pl.CostEstimate(flops=own.size * 8, bytes_accessed=own.size * 8, transcendentals=0),
        name="total",
    )(own, *codes)


def place(own, codes, other):
    vmem = pl.BlockSpec(memory_space=pltpu.VMEM)
    return pl.pallas_call(
        place_kernel,
        in_specs=[vmem] * (2 + len(codes)),
        out_specs=vmem,
        out_shape=jax.ShapeDtypeStruct((2, *own.shape), jnp.float32),
        cost_estimate=pl.CostEstimate(flops=own.size * 8, bytes_accessed=own.size * 8, transcendentals=0),
        name="place",
    )(own, *codes, other)


def shards(x_rows, dy_rows, seg_blocks):
    rows, hid = x_rows.shape
    ffn = dy_rows.shape[1]
    n_exp = lax.axis_size("expert")
    n_dp = lax.axis_size("dp")
    nblk = rows // BLOCK
    cap = min(CAP, nblk)
    blk = hid // n_dp
    nz = n_dp // 4
    piece = ffn // n_exp
    per_chunk = n_exp // CHUNKS
    fc = ffn // CHUNKS

    swap = [(i, i ^ 1) for i in range(n_dp)]
    over_x = [(i, i ^ 2) for i in range(n_dp)]

    def ring(n, j):
        return [(i, (i + j) % n) for i in range(n)]

    own, *sends = pack(seg_blocks, x_rows, dy_rows, n_exp, cap)
    heads = [lax.ppermute(sends[2 * j - 2], "expert", ring(n_exp, j)) for j in range(1, n_exp)]
    tails = [lax.ppermute(sends[2 * j - 1], "expert", ring(n_exp, j)) for j in range(1, n_exp)]
    own_pair = [own, lax.ppermute(own, "dp", swap)]
    head_pairs = []
    for head in heads:
        head_pairs += [head, lax.ppermute(head, "dp", swap)]

    got, left, codes = [], None, []
    for chunk in range(CHUNKS):
        dys = [(a, hid + chunk * fc) for a in own_pair]
        if chunk == 0:
            dys += [(a, hid) for a in head_pairs]
            code, keep, left = product(
                seg_blocks, None, own_pair + head_pairs, dys, n_exp, nblk, nz, blk, hid, fc
            )
        else:
            code0, *tails = lax.optimization_barrier((codes[0][0], *tails))
            codes[0] = (code0, codes[0][1])
            for tail in tails:
                dys += [(tail, 0), (lax.ppermute(tail, "dp", swap), 0)]
            code, keep = product(seg_blocks, left, None, dys, n_exp, nblk, nz, blk, hid, fc)
        codes.append((code, keep))
    for chunk in range(CHUNKS):
        code, keep = codes[chunk]
        code = lax.ppermute(code, "dp", over_x)
        *parts, own = middle(code, keep, nz, blk)
        parts = [lax.ppermute(part, "dp", ring(n_dp, 4 * (j + 1))) for j, part in enumerate(parts)]
        if n_exp == 2 and chunk == CHUNKS - 1:
            return place(own, parts, got[0])
        result = total(own, parts)
        for p in range(per_chunk):
            shift = 1 + chunk * per_chunk + p
            part = result[:, p * piece : (p + 1) * piece]
            got.append(lax.ppermute(part, "expert", ring(n_exp, shift)) if shift < n_exp else part)
    order = (lax.axis_index("expert") - 1 - jnp.arange(n_exp)) % n_exp
    return jnp.stack(got)[order]


def solution(mesh):
    in_specs = (P(("dp", "expert"), None), P(("dp", "expert"), None), P())
    out_specs = P(None, "dp", "expert")
    return jax.shard_map(shards, mesh=mesh, in_specs=in_specs, out_specs=out_specs, check_vma=False)
```
